32 devices in a mesh: ctx: 8 (over y, x, core), fsdp: 4 (over z).
Axes of the slice: x: 2, y: 2, z: 4, core: 2. Of those that a mesh axis runs over, the one named last changes fastest.
Arguments:
- tokens: bfloat16 [4, 1024, 2048], P('fsdp', 'ctx'), may hold values from -70 to 70
- block_order: int32 [4, 16], P('fsdp'), may hold values from 0 to 15, each once within a row
- w_query: bfloat16 [2048, 2048], P('fsdp')
- w_key: bfloat16 [2048, 2048], P('fsdp'), may hold values from -2 to 2
- w_value: bfloat16 [2048, 2048], P('fsdp'), may hold values from -0.125 to 0.125
- w_out: bfloat16 [2048, 2048], P('fsdp'), may hold values from -2 to 2
- w_gate: bfloat16 [2048, 8192], P('fsdp'), may hold values from -0.125 to 0.125
- w_up: bfloat16 [2048, 8192], P('fsdp'), may hold values from -0.125 to 0.125
- w_down: bfloat16 [2048, 8192], P('fsdp'), may hold values from -0.0625 to 0.0625
- norm_attn: bfloat16 [2048], P('fsdp'), may hold values from 0.5 to 1.5
- norm_mlp: bfloat16 [2048], P('fsdp'), may hold values from 0.5 to 1.5
- cotangent: bfloat16 [4, 1024, 2048], P('fsdp', 'ctx'), may hold values from -6 to 6
Outputs:
- output: float32 [4, 1024, 2048], P('fsdp', 'ctx')
- grad_tokens: float32 [4, 1024, 2048], P('fsdp', 'ctx')
- grad_query: float32 [2048, 2048], P('fsdp', 'ctx')
- grad_key: float32 [2048, 2048], P('fsdp', 'ctx')
- grad_value: float32 [2048, 2048], P('fsdp', 'ctx')
- grad_out: float32 [2048, 2048], P('fsdp', 'ctx')
- grad_gate: float32 [2048, 8192], P('fsdp', 'ctx')
- grad_up: float32 [2048, 8192], P('fsdp', 'ctx')
- grad_down: float32 [2048, 8192], P('fsdp', 'ctx')
- grad_norm_attn: float32 [2048], P('fsdp')
- grad_norm_mlp: float32 [2048], P('fsdp')
The draws below stay inside these ranges and needn't reach their ends.
Inputs may be any that keep to these rules, and one draw needn't show every extreme that they name: `block_order`: each row lists each of the 16 blocks of its sequence once.
All inputs are finite; a program needn't handle non-finite values.
Results may differ from the reference program's by a relative error of at most 0.018.
Values may be sent and summed in bfloat16 or wider, within the bound.
A program may use at most 448 MiB of HBM per device.

```python
import jax
import jax.numpy as jnp
from jax import lax

D = 2048
HEADS = 32
HD = 64
FF = 8192
TOK_DEV = 128
SEQ_LEN = 1024
SEQS = 4
BLK = 64
BLOCKS = 16


def query_key_pair(key):
    base = jax.random.fold_in(key, 11)
    first, second = jax.random.split(base, 2)
    scaling = D ** (-0.5)
    query_draw = jnp.clip(jax.random.normal(first, (D, D), jnp.float32), -4.0, 4.0) * scaling
    key_draw = jnp.clip(jax.random.normal(second, (D, D), jnp.float32), -4.0, 4.0) * scaling
    return (query_draw, key_draw)


def draw_w_query(key, part):
    return query_key_pair(key)[0].astype(jnp.bfloat16)


def draw_w_key(key, part):
    return query_key_pair(key)[1].astype(jnp.bfloat16)


def draw_tokens(key, part):
    first, second, third = jax.random.split(jax.random.fold_in(key, 23), 3)
    base = jnp.clip(jax.random.normal(first, (SEQS, SEQ_LEN, D), jnp.float32), -6.0, 6.0)
    row_scale = jnp.exp(jax.random.uniform(second, (SEQS, SEQ_LEN, 1), jnp.float32, -1.2, 1.2))
    column_scale = jnp.exp(jax.random.uniform(third, (1, 1, D), jnp.float32, -1.2, 1.2))
    return (base * row_scale * column_scale).astype(jnp.bfloat16)


def block_levels(key, extent, cuts, smallest, largest):
    def one(position, blocks):
        steps = jax.random.uniform(jax.random.fold_in(jax.random.fold_in(key, 6), position), (blocks,), jnp.float32, smallest / len(cuts), largest / len(cuts))
        return jnp.repeat(jnp.exp(steps), extent[position] // blocks).reshape((-1,) + (1,) * (len(extent) - position - 1))

    loudness = one(*cuts[0])
    for cut in cuts[1:]:
        loudness = loudness * one(*cut)
    return loudness


def normal_values(stream_key, extent, deviation, limit, cuts=(), kind=jnp.bfloat16):
    array = deviation * jax.random.normal(stream_key, extent, jnp.float32)
    if cuts:
        array = array * block_levels(stream_key, extent, cuts, -0.22, 0.18)
    return jnp.clip(array, -limit, limit).astype(kind)


def setup_inputs(seed: int = 0) -> dict:
    streams_of = jax.random.split(jax.random.key(seed), 13)
    tokens = draw_tokens(jax.random.fold_in(streams_of[12], 71), 0)
    block_order = jax.vmap(lambda own: jax.random.permutation(own, BLOCKS))(jax.random.split(streams_of[1], SEQS)).reshape((SEQS, BLOCKS)).astype(jnp.int32)
    w_query = draw_w_query(jax.random.fold_in(streams_of[12], 71), 0)
    w_key = draw_w_key(jax.random.fold_in(streams_of[12], 71), 0)
    w_value = normal_values(streams_of[4], (D, D), D ** -0.5, 0.125, ((0, 4),))
    w_out = normal_values(streams_of[5], (D, D), 8 ** -0.5, 2.0, ((0, 4),))
    w_gate = normal_values(streams_of[6], (D, FF), D ** -0.5, 0.125, ((0, 4),))
    w_up = normal_values(streams_of[7], (D, FF), D ** -0.5, 0.125, ((0, 4),))
    w_down = normal_values(streams_of[8], (D, FF), FF ** -0.5, 0.0625, ((0, 4),))
    norm_attn = jnp.clip(1.0 + 0.1 * jax.random.normal(streams_of[9], (D,), jnp.float32), 0.5, 1.5).astype(jnp.bfloat16)
    norm_mlp = jnp.clip(1.0 + 0.1 * jax.random.normal(streams_of[10], (D,), jnp.float32), 0.5, 1.5).astype(jnp.bfloat16)
    cotangent = normal_values(streams_of[11], (SEQS, SEQ_LEN, D), 1.0, 6.0, ((0, 4), (1, 8)))
    return {"tokens": tokens, "block_order": block_order, "w_query": w_query, "w_key": w_key, "w_value": w_value, "w_out": w_out, "w_gate": w_gate, "w_up": w_up, "w_down": w_down, "norm_attn": norm_attn, "norm_mlp": norm_mlp, "cotangent": cotangent}


eps = 1e-05
rope_base = 130000.0
neg_large = -1e+30

def rms_scale(values):
    return lax.rsqrt(lax.optimization_barrier(jnp.mean(values * values, axis=-1, keepdims=True)) + eps)

def norm_back(grad_normed, normed, scaling):
    return scaling * (grad_normed - normed * lax.optimization_barrier(jnp.mean(grad_normed * normed, axis=-1, keepdims=True)))

def rounded(values):
    return lax.optimization_barrier(values.astype(jnp.bfloat16)).astype(jnp.float32)

def rotation_tables(positions, head_size):
    half_size = head_size // 2
    freqs = rope_base ** (-(jnp.arange(half_size, dtype=jnp.float32) * (2.0 / head_size)))
    angles = positions.astype(jnp.float32)[:, None] * freqs[None, :]
    cosine = jnp.concatenate([jnp.cos(angles), jnp.cos(angles)], axis=-1)[:, None, :]
    sine = jnp.concatenate([jnp.sin(angles), jnp.sin(angles)], axis=-1)[:, None, :]
    return (cosine, sine)

def rotate(values, cosine, sine):
    half_size = values.shape[-1] // 2
    turned = jnp.concatenate([-values[..., half_size:], values[..., :half_size]], axis=-1)
    return values * cosine + turned * sine

def rotate_back(grads, cosine, sine):
    half_size = grads.shape[-1] // 2
    scaled = grads * sine
    turned = jnp.concatenate([scaled[..., half_size:], -scaled[..., :half_size]], axis=-1)
    return grads * cosine + turned

def one_sequence(x_seq, order_seq, dy_seq, w_query, w_key, w_value, w_out, w_gate, w_up, w_down, norm_attn, norm_mlp):
    seq_rows = x_seq.shape[0]
    width = x_seq.shape[1]
    scaling = HD ** (-0.5)
    row_ids = jnp.arange(seq_rows, dtype=jnp.int32)
    positions = order_seq[row_ids // BLK].astype(jnp.int32) * BLK + row_ids % BLK
    xs = x_seq.astype(jnp.float32)
    scale_attn = rms_scale(xs)
    normed_attn = xs * scale_attn
    hidden_attn = (normed_attn * norm_attn.astype(jnp.float32)[None, :]).astype(jnp.bfloat16)
    query = jnp.dot(hidden_attn, w_query, preferred_element_type=jnp.float32)
    keyed = jnp.dot(hidden_attn, w_key, preferred_element_type=jnp.float32)
    valued = jnp.dot(hidden_attn, w_value, preferred_element_type=jnp.float32)
    cosine, sine = rotation_tables(positions, HD)
    query_rot = rotate(query.reshape(seq_rows, HEADS, HD), cosine, sine).astype(jnp.bfloat16)
    key_rot = rotate(keyed.reshape(seq_rows, HEADS, HD), cosine, sine).astype(jnp.bfloat16)
    value_b = valued.reshape(seq_rows, HEADS, HD).astype(jnp.bfloat16)
    key_f = key_rot.astype(jnp.float32)
    value_f = value_b.astype(jnp.float32)
    query_blocks = seq_rows // TOK_DEV

    def forward_block(block_id):
        first_row = block_id * TOK_DEV
        q_block = lax.dynamic_slice_in_dim(query_rot, first_row, TOK_DEV, 0).astype(jnp.float32)
        q_pos = lax.dynamic_slice_in_dim(positions, first_row, TOK_DEV, 0)
        scores = jnp.einsum('qhd,khd->hqk', q_block, key_f) * scaling
        allowed = (positions[None, :] <= q_pos[:, None])[None]
        maxima = lax.optimization_barrier(jnp.max(jnp.where(allowed, scores, neg_large), axis=-1))
        probs = jnp.where(allowed, jnp.exp(scores - maxima[..., None]), 0.0)
        totals = lax.optimization_barrier(jnp.sum(probs, axis=-1))
        rows_out = jnp.einsum('hqk,khd->qhd', rounded(probs), value_f) / totals.T[:, :, None]
        return (rows_out, maxima + jnp.log(totals))
    attn_blocks, lse_blocks = lax.map(forward_block, jnp.arange(query_blocks, dtype=jnp.int32))
    attn_rows = attn_blocks.reshape(seq_rows, width).astype(jnp.bfloat16)
    mid_stream = xs + jnp.dot(attn_rows, w_out, preferred_element_type=jnp.float32)
    scale_mlp = rms_scale(mid_stream)
    normed_mlp = mid_stream * scale_mlp
    hidden_mlp = (normed_mlp * norm_mlp.astype(jnp.float32)[None, :]).astype(jnp.bfloat16)
    gate_pre = jnp.dot(hidden_mlp, w_gate, preferred_element_type=jnp.float32)
    up_pre = jnp.dot(hidden_mlp, w_up, preferred_element_type=jnp.float32)
    sigmoid_gate = jax.nn.sigmoid(gate_pre)
    silu_gate = gate_pre * sigmoid_gate
    acted = (silu_gate * up_pre).astype(jnp.bfloat16)
    output = mid_stream + jnp.dot(acted, w_down.T, preferred_element_type=jnp.float32)
    grad_b = dy_seq
    grad_down = jnp.dot(grad_b.T, acted, preferred_element_type=jnp.float32)
    grad_act = jnp.dot(grad_b, w_down, preferred_element_type=jnp.float32)
    grad_gate_pre = (grad_act * up_pre * sigmoid_gate * (1.0 + gate_pre * (1.0 - sigmoid_gate))).astype(jnp.bfloat16)
    grad_up_pre = (grad_act * silu_gate).astype(jnp.bfloat16)
    grad_gate = jnp.dot(hidden_mlp.T, grad_gate_pre, preferred_element_type=jnp.float32)
    grad_up = jnp.dot(hidden_mlp.T, grad_up_pre, preferred_element_type=jnp.float32)
    grad_hidden_mlp = jnp.dot(grad_gate_pre, w_gate.T, preferred_element_type=jnp.float32) + jnp.dot(grad_up_pre, w_up.T, preferred_element_type=jnp.float32)
    grad_norm_mlp = lax.optimization_barrier(jnp.sum(grad_hidden_mlp * normed_mlp, axis=0))
    grad_mid = grad_b.astype(jnp.float32) + norm_back(grad_hidden_mlp * norm_mlp.astype(jnp.float32)[None, :], normed_mlp, scale_mlp)
    grad_mid_b = grad_mid.astype(jnp.bfloat16)
    grad_out = jnp.dot(attn_rows.T, grad_mid_b, preferred_element_type=jnp.float32)
    grad_attn = jnp.dot(grad_mid_b, w_out.T, preferred_element_type=jnp.float32).astype(jnp.bfloat16)
    grad_attn_f = grad_attn.astype(jnp.float32).reshape(seq_rows, HEADS, HD)
    delta = lax.optimization_barrier(jnp.sum(grad_attn_f * attn_rows.astype(jnp.float32).reshape(seq_rows, HEADS, HD), axis=-1))

    def backward_block(carried, block_id):
        grad_k_acc, grad_v_acc = carried
        first_row = block_id * TOK_DEV
        q_block = lax.dynamic_slice_in_dim(query_rot, first_row, TOK_DEV, 0).astype(jnp.float32)
        q_pos = lax.dynamic_slice_in_dim(positions, first_row, TOK_DEV, 0)
        do_block = lax.dynamic_slice_in_dim(grad_attn_f, first_row, TOK_DEV, 0)
        lse_block = lse_blocks[block_id]
        delta_block = lax.dynamic_slice_in_dim(delta, first_row, TOK_DEV, 0)
        scores = jnp.einsum('qhd,khd->hqk', q_block, key_f) * scaling
        allowed = (positions[None, :] <= q_pos[:, None])[None]
        probs = jnp.where(allowed, jnp.exp(scores - lse_block[..., None]), 0.0)
        grad_v_acc = grad_v_acc + jnp.einsum('hqk,qhd->khd', rounded(probs), do_block)
        grad_probs = jnp.einsum('qhd,khd->hqk', do_block, value_f)
        grad_scores = rounded(probs * (grad_probs - delta_block.T[:, :, None]) * scaling)
        grad_q_block = jnp.einsum('hqk,khd->qhd', grad_scores, key_f)
        grad_k_acc = grad_k_acc + jnp.einsum('hqk,qhd->khd', grad_scores, q_block)
        return ((grad_k_acc, grad_v_acc), grad_q_block)
    zeros_heads = jnp.zeros((seq_rows, HEADS, HD), jnp.float32)
    (grad_kr, grad_vb), grad_q_blocks = lax.scan(backward_block, (zeros_heads, zeros_heads), jnp.arange(query_blocks, dtype=jnp.int32))
    grad_qr = grad_q_blocks.reshape(seq_rows, HEADS, HD)
    grad_q = rotate_back(grad_qr, cosine, sine).reshape(seq_rows, width).astype(jnp.bfloat16)
    grad_k = rotate_back(grad_kr, cosine, sine).reshape(seq_rows, width).astype(jnp.bfloat16)
    grad_v = grad_vb.reshape(seq_rows, width).astype(jnp.bfloat16)
    grad_query = jnp.dot(hidden_attn.T, grad_q, preferred_element_type=jnp.float32)
    grad_key = jnp.dot(hidden_attn.T, grad_k, preferred_element_type=jnp.float32)
    grad_value = jnp.dot(hidden_attn.T, grad_v, preferred_element_type=jnp.float32)
    grad_hidden_attn = jnp.dot(grad_q, w_query.T, preferred_element_type=jnp.float32) + jnp.dot(grad_k, w_key.T, preferred_element_type=jnp.float32) + jnp.dot(grad_v, w_value.T, preferred_element_type=jnp.float32)
    grad_norm_attn = lax.optimization_barrier(jnp.sum(grad_hidden_attn * normed_attn, axis=0))
    grad_tokens = grad_mid + norm_back(grad_hidden_attn * norm_attn.astype(jnp.float32)[None, :], normed_attn, scale_attn)
    grads = (grad_query, grad_key, grad_value, grad_out, grad_gate, grad_up, grad_down, grad_norm_attn, grad_norm_mlp)
    return (output, grad_tokens, grads)

def reference(tokens, block_order, w_query, w_key, w_value, w_out, w_gate, w_up, w_down, norm_attn, norm_mlp, cotangent):
    shapes = (w_query, w_key, w_value, w_out, w_gate, w_up, w_down, norm_attn, norm_mlp)

    def per_sequence(carried, inputs_seq):
        x_seq, order_seq, dy_seq = inputs_seq
        output, grad_tokens, grads = one_sequence(x_seq, order_seq, dy_seq, w_query, w_key, w_value, w_out, w_gate, w_up, w_down, norm_attn, norm_mlp)
        return (tuple((total + part for total, part in zip(carried, grads))), (output, grad_tokens))
    initial = tuple((jnp.zeros(weight.shape, jnp.float32) for weight in shapes))
    summed, (outputs, grad_inputs) = lax.scan(per_sequence, initial, (tokens, block_order, cotangent))
    return (outputs, grad_inputs, summed[0], summed[1], summed[2], summed[3], summed[4], summed[5], summed[6], summed[7], summed[8])
```

```python
import jax
import jax.numpy as jnp
from jax import lax
from jax.sharding import PartitionSpec as P

HEADS = 32
HD = 64


eps = 1e-05
rope_base = 130000.0
neg_large = -1e30


def rms_scale(values):
    return lax.rsqrt(jnp.mean(values * values, axis=-1, keepdims=True) + eps)


def norm_back(grad_normed, normed, scaling):
    return scaling * (grad_normed - normed * jnp.mean(grad_normed * normed, axis=-1, keepdims=True))


def slot_positions(layout, row_ids, half_rows):
    slots = row_ids // half_rows
    onehot = slots[:, None] == jnp.arange(layout.shape[0], dtype=jnp.int32)[None, :]
    return jnp.sum(jnp.where(onehot, layout[None, :], 0), axis=1) * half_rows + row_ids % half_rows


def rotation_tables(positions, head_size):
    half_size = head_size // 2
    freqs = rope_base ** (-(jnp.arange(half_size, dtype=jnp.float32) * (2.0 / head_size)))
    angles = positions.astype(jnp.float32)[:, None] * freqs[None, :]
    cosine = jnp.concatenate([jnp.cos(angles), jnp.cos(angles)], axis=-1)[:, None, :]
    sine = jnp.concatenate([jnp.sin(angles), jnp.sin(angles)], axis=-1)[:, None, :]
    return (cosine, sine)


def rotate(values, cosine, sine):
    half_size = values.shape[-1] // 2
    turned = jnp.concatenate([-values[..., half_size:], values[..., :half_size]], axis=-1)
    return values * cosine + turned * sine


def rotate_back(grads, cosine, sine):
    half_size = grads.shape[-1] // 2
    scaled = grads * sine
    turned = jnp.concatenate([scaled[..., half_size:], -scaled[..., :half_size]], axis=-1)
    return grads * cosine + turned


def contract_last(left, right):
    return lax.dot_general(
        left, right, (((1,), (1,)), ((), ())), preferred_element_type=jnp.float32
    )


def own_columns(weight, place, size):
    share = weight.shape[1] // size
    return lax.dynamic_slice_in_dim(weight, place * share, share, 1)


def rows_gathered(part):
    return lax.all_gather(part, "fsdp", axis=0, tiled=True)


def contract_rows(left, right):
    return lax.dot_general(
        left, right, (((0,), (0,)), ((), ())), preferred_element_type=jnp.float32
    )


def plane_gather(part):
    return lax.all_gather(part, "ctx", axis=0, tiled=True)


def plane_scatter(total):
    return lax.psum_scatter(total.astype(jnp.bfloat16), "ctx", scatter_dimension=0, tiled=True).astype(
        jnp.float32
    )


def grads_scattered(total):
    return lax.psum_scatter(
        total.astype(jnp.bfloat16), "fsdp", scatter_dimension=0, tiled=True
    ).astype(jnp.float32)


def on_device(
    tokens,
    block_order,
    w_query,
    w_key,
    w_value,
    w_out,
    w_gate,
    w_up,
    w_down,
    norm_attn,
    norm_mlp,
    cotangent,
):
    inputs = tokens[0].astype(jnp.float32)
    tok_rows, model_width = inputs.shape
    head_size = HD
    scaling = head_size ** (-0.5)
    layout = block_order[0]
    ctx_size = lax.axis_size("ctx")
    ctx_place = lax.axis_index("ctx")
    fsdp_size = lax.axis_size("fsdp")
    fsdp_place = lax.axis_index("fsdp")
    seq_rows = tok_rows * ctx_size
    block_rows = seq_rows // layout.shape[0]
    own_heads = HEADS // ctx_size
    share = model_width // ctx_size
    positions = slot_positions(layout, jnp.arange(seq_rows, dtype=jnp.int32), block_rows)
    cosine, sine = rotation_tables(positions, head_size)

    gains = rows_gathered(jnp.stack([norm_attn, norm_mlp], axis=1)).astype(jnp.float32)
    gain_attn, gain_mlp = gains[:, 0], gains[:, 1]
    w_qkv = rows_gathered(
        jnp.concatenate([own_columns(w, ctx_place, ctx_size) for w in (w_query, w_key, w_value)], axis=1)
    )
    out_cols = rows_gathered(own_columns(w_out, ctx_place, ctx_size))
    out_rows = lax.all_to_all(out_cols, "ctx", split_axis=0, concat_axis=1, tiled=True)
    gate_cols = rows_gathered(own_columns(w_gate, ctx_place, ctx_size))
    up_cols = rows_gathered(own_columns(w_up, ctx_place, ctx_size))
    down_cols = rows_gathered(own_columns(w_down, ctx_place, ctx_size))

    scale_attn = rms_scale(inputs)
    normed_attn = inputs * scale_attn
    hidden_attn = plane_gather((normed_attn * gain_attn[None, :]).astype(jnp.bfloat16))
    grad_b = plane_gather(cotangent[0])
    qkv = jnp.dot(hidden_attn, w_qkv, preferred_element_type=jnp.float32)
    by_head = qkv.reshape(seq_rows, 3, own_heads, head_size)
    query_rot = rotate(by_head[:, 0], cosine, sine).astype(jnp.bfloat16)
    key_rot = rotate(by_head[:, 1], cosine, sine).astype(jnp.bfloat16)
    value_b = by_head[:, 2].astype(jnp.bfloat16)
    allowed = (positions[None, :] <= positions[:, None])[None]
    scores = jnp.einsum("qhd,khd->hqk", query_rot, key_rot, preferred_element_type=jnp.float32) * scaling
    maxima = jnp.max(jnp.where(allowed, scores, neg_large), axis=-1)
    probs = jnp.where(allowed, jnp.exp(scores - maxima[..., None]), 0.0)
    totals = jnp.sum(probs, axis=-1)
    mixed = jnp.einsum("hqk,khd->qhd", probs.astype(jnp.bfloat16), value_b, preferred_element_type=jnp.float32)
    attn_rows = (mixed / totals.T[:, :, None]).astype(jnp.bfloat16).reshape(seq_rows, share)
    log_totals = maxima + jnp.log(totals)

    mid_stream = inputs + plane_scatter(jnp.dot(attn_rows, out_rows, preferred_element_type=jnp.float32))
    scale_mlp = rms_scale(mid_stream)
    normed_mlp = mid_stream * scale_mlp
    hidden_mlp = plane_gather((normed_mlp * gain_mlp[None, :]).astype(jnp.bfloat16))
    gate_pre = jnp.dot(hidden_mlp, gate_cols, preferred_element_type=jnp.float32)
    up_pre = jnp.dot(hidden_mlp, up_cols, preferred_element_type=jnp.float32)
    sigmoid_gate = jax.nn.sigmoid(gate_pre)
    silu_gate = gate_pre * sigmoid_gate
    acted = (silu_gate * up_pre).astype(jnp.bfloat16)
    result = mid_stream + plane_scatter(contract_last(acted, down_cols))
    grad_down = grads_scattered(contract_rows(grad_b, acted))

    grad_act = jnp.dot(grad_b, down_cols, preferred_element_type=jnp.float32)
    grad_gate_pre = (
        grad_act * up_pre * sigmoid_gate * (1.0 + gate_pre * (1.0 - sigmoid_gate))
    ).astype(jnp.bfloat16)
    grad_up_pre = (grad_act * silu_gate).astype(jnp.bfloat16)
    grad_gate = grads_scattered(contract_rows(hidden_mlp, grad_gate_pre))
    grad_up = grads_scattered(contract_rows(hidden_mlp, grad_up_pre))
    columns = plane_scatter(contract_last(grad_gate_pre, gate_cols) + contract_last(grad_up_pre, up_cols))
    gain_grad_mlp = jnp.sum(columns * normed_mlp, axis=0)
    grad_mid = cotangent[0].astype(jnp.float32) + norm_back(
        columns * gain_mlp[None, :], normed_mlp, scale_mlp
    )
    grad_mid_b = plane_gather(grad_mid.astype(jnp.bfloat16))
    attn_all = lax.all_gather(attn_rows, "ctx", axis=1, tiled=True)
    grad_out = grads_scattered(contract_rows(attn_all, own_columns(grad_mid_b, ctx_place, ctx_size)))
    grad_attn = contract_last(grad_mid_b, out_rows).astype(jnp.bfloat16)
    delta = jnp.sum(
        (grad_attn.astype(jnp.float32) * attn_rows.astype(jnp.float32)).reshape(
            seq_rows, own_heads, head_size
        ),
        axis=-1,
    ).T
    grad_heads = grad_attn.reshape(seq_rows, own_heads, head_size)
    probs = jnp.where(allowed, jnp.exp(scores - log_totals[..., None]), 0.0)
    grad_v = jnp.einsum("hqk,qhd->khd", probs.astype(jnp.bfloat16), grad_heads, preferred_element_type=jnp.float32)
    grad_probs = jnp.einsum("qhd,khd->hqk", grad_heads, value_b, preferred_element_type=jnp.float32)
    grad_scores = (probs * (grad_probs - delta[..., None]) * scaling).astype(jnp.bfloat16)
    grad_q = jnp.einsum("hqk,khd->qhd", grad_scores, key_rot, preferred_element_type=jnp.float32)
    grad_k = jnp.einsum("hqk,qhd->khd", grad_scores, query_rot, preferred_element_type=jnp.float32)
    grad_qkv = jnp.stack(
        [
            rotate_back(grad_q, cosine, sine).astype(jnp.bfloat16),
            rotate_back(grad_k, cosine, sine).astype(jnp.bfloat16),
            grad_v.astype(jnp.bfloat16),
        ],
        axis=1,
    ).reshape(seq_rows, 3 * share)
    columns = plane_scatter(contract_last(grad_qkv, w_qkv))
    grads_qkv = grads_scattered(contract_rows(hidden_attn, grad_qkv))
    gain_grad_attn = jnp.sum(columns * normed_attn, axis=0)
    grad_input = grad_mid + norm_back(columns * gain_attn[None, :], normed_attn, scale_attn)
    gain_own = lax.psum(
        lax.psum_scatter(jnp.stack([gain_grad_attn, gain_grad_mlp], axis=1), "fsdp", scatter_dimension=0, tiled=True),
        "ctx",
    )
    return (
        result[None],
        grad_input[None],
        grads_qkv[:, :share],
        grads_qkv[:, share : 2 * share],
        grads_qkv[:, 2 * share :],
        grad_out,
        grad_gate,
        grad_up,
        grad_down,
        gain_own[:, 0],
        gain_own[:, 1],
    )


def solution(mesh):
    in_specs = (
        P("fsdp", "ctx", None),
        P("fsdp", None),
        P("fsdp", None),
        P("fsdp", None),
        P("fsdp", None),
        P("fsdp", None),
        P("fsdp", None),
        P("fsdp", None),
        P("fsdp", None),
        P("fsdp"),
        P("fsdp"),
        P("fsdp", "ctx", None),
    )
    out_specs = (
        P("fsdp", "ctx", None),
        P("fsdp", "ctx", None),
        P("fsdp", "ctx"),
        P("fsdp", "ctx"),
        P("fsdp", "ctx"),
        P("fsdp", "ctx"),
        P("fsdp", "ctx"),
        P("fsdp", "ctx"),
        P("fsdp", "ctx"),
        P("fsdp"),
        P("fsdp"),
    )
    return jax.shard_map(
        on_device, mesh=mesh, in_specs=in_specs, out_specs=out_specs, check_vma=False
    )
```

```python
import jax
import jax.numpy as jnp
from jax import lax
from jax.experimental import pallas as pl
from jax.experimental.pallas import tpu as pltpu
from jax.sharding import PartitionSpec as P


HEADS = 32
HD = 64


eps = 1e-05
rope_base = 130000.0
neg_large = -1e30


def rms_scale(values):
    return lax.rsqrt(jnp.mean(values * values, axis=-1, keepdims=True) + eps)


def norm_back(grad_normed, normed, scaling):
    return scaling * (grad_normed - normed * jnp.mean(grad_normed * normed, axis=-1, keepdims=True))


def slot_positions(layout, row_ids, half_rows):
    slots = row_ids // half_rows
    onehot = slots[:, None] == jnp.arange(layout.shape[0], dtype=jnp.int32)[None, :]
    return jnp.sum(jnp.where(onehot, layout[None, :], 0), axis=1) * half_rows + row_ids % half_rows


def rotation_tables(positions, head_size):
    half_size = head_size // 2
    freqs = rope_base ** (-(jnp.arange(half_size, dtype=jnp.float32) * (2.0 / head_size)))
    angles = positions.astype(jnp.float32)[:, None] * freqs[None, :]
    cosine = jnp.concatenate([jnp.cos(angles), jnp.cos(angles)], axis=-1)[:, None, :]
    sine = jnp.concatenate([jnp.sin(angles), jnp.sin(angles)], axis=-1)[:, None, :]
    return (cosine, sine)


def rotate(values, cosine, sine):
    half_size = values.shape[-1] // 2
    turned = jnp.concatenate([-values[..., half_size:], values[..., :half_size]], axis=-1)
    return values * cosine + turned * sine


def rotate_back(grads, cosine, sine):
    half_size = grads.shape[-1] // 2
    scaled = grads * sine
    turned = jnp.concatenate([scaled[..., half_size:], -scaled[..., :half_size]], axis=-1)
    return grads * cosine + turned


def contract_last(left, right):
    return lax.dot_general(
        left, right, (((1,), (1,)), ((), ())), preferred_element_type=jnp.float32
    )


def own_columns(weight, place, size):
    share = weight.shape[1] // size
    return lax.dynamic_slice_in_dim(weight, place * share, share, 1)


def rows_gathered(part):
    return lax.all_gather(part, "fsdp", axis=0, tiled=True)


def contract_rows(left, right):
    return lax.dot_general(
        left, right, (((0,), (0,)), ((), ())), preferred_element_type=jnp.float32
    )


def send(source, target, sems, slot, peer):
    send_sems, recv_sems = sems
    return pltpu.make_async_remote_copy(
        src_ref=source,
        dst_ref=target,
        send_sem=send_sems.at[slot],
        recv_sem=recv_sems.at[slot],
        device_id=peer,
        device_id_type=pl.DeviceIdType.MESH,
    )


def greet(peers):
    barrier = pltpu.get_barrier_semaphore()
    for peer in peers:
        pl.semaphore_signal(barrier, inc=1, device_id=peer, device_id_type=pl.DeviceIdType.MESH)
    pl.semaphore_wait(barrier, len(peers))


def plane_peers():
    me = lax.axis_index("ctx")
    z = lax.axis_index("fsdp")
    return me, z, (me ^ 1, z), (me ^ 2, z), (me ^ 4, z)


def gather_copies(part, whole, me, core, x, y, sems, base):
    half = part.shape[0] // 2
    first, last = pl.ds(0, half), pl.ds(half, half)

    def block(owner, rows):
        return whole.at[owner, rows]

    own = [
        send(part.at[first], block(me, first), sems, base + 0, y),
        send(part.at[last], block(me, last), sems, base + 1, x),
        send(part.at[last], block(me, last), sems, base + 2, y),
        send(part.at[first], block(me, first), sems, base + 3, x),
        send(part, whole.at[me], sems, base + 4, core),
    ]
    along_x = send(block(me ^ 4, first), block(me ^ 4, first), sems, base + 5, x)
    along_y = send(block(me ^ 2, last), block(me ^ 2, last), sems, base + 6, y)
    to_core = [
        send(whole.at[me ^ 4], whole.at[me ^ 4], sems, base + 7, core),
        send(whole.at[me ^ 2], whole.at[me ^ 2], sems, base + 8, core),
        send(block(me ^ 6, first), block(me ^ 6, first), sems, base + 9, core),
        send(block(me ^ 6, last), block(me ^ 6, last), sems, base + 10, core),
    ]
    return own, along_x, along_y, to_core


GATHER_COPIES = 11


def plane_gather_steps(parts, wholes, place, sems, kept_sems):
    me, _, core, x, y = place
    plans = [
        gather_copies(parts[i], wholes[i], me, core, x, y, sems, i * GATHER_COPIES) for i in range(len(parts))
    ]
    kept = [
        pltpu.make_async_copy(parts[i], wholes[i].at[me], kept_sems.at[i]) for i in range(len(parts))
    ]

    def begin():
        for plan in plans:
            for copy in plan[0]:
                copy.start()
        for copy in kept:
            copy.start()

    def turn(own, along_x, along_y, to_core):
        own[0].wait_recv()
        along_x.start()
        own[1].wait_recv()
        along_y.start()
        own[2].wait_recv()
        to_core[0].start()
        own[3].wait_recv()
        to_core[1].start()

    def share(own, along_x, along_y, to_core):
        along_x.wait_recv()
        to_core[2].start()
        along_y.wait_recv()
        to_core[3].start()

    def end():
        for own, along_x, along_y, to_core in plans:
            own[4].wait_recv()
            for copy in to_core:
                copy.wait_recv()
            for copy in own + [along_x, along_y] + to_core:
                copy.wait_send()
        for copy in kept:
            copy.wait()

    steps = [begin]
    steps += [lambda plan=plan: turn(*plan) for plan in plans]
    steps += [lambda plan=plan: share(*plan) for plan in plans]
    return steps, end


def line_gather_steps(size, parts, wholes, place, sems, kept_sems):
    ctx, me = place[0], place[1]
    send_sems, recv_sems = sems
    kept = [
        pltpu.make_async_copy(parts[i], wholes[i].at[me], kept_sems.at[i]) for i in range(len(parts))
    ]

    def passing(i, upward, dist, source, owner):
        return pltpu.make_async_remote_copy(
            src_ref=source,
            dst_ref=wholes[i].at[owner],
            send_sem=send_sems.at[i, upward, dist],
            recv_sem=recv_sems.at[i, upward, dist],
            device_id=(ctx, me + (1 if upward else -1)),
            device_id_type=pl.DeviceIdType.MESH,
        )

    def sends(upward, dist):
        return ((me < size - 1) & (me >= dist - 1)) if upward else ((me > 0) & (me <= size - dist))

    def step(dist):
        for i in range(len(parts)):
            for upward in (1, 0):
                owner = me - (dist - 1) if upward else me + (dist - 1)

                @pl.when(sends(upward, dist))
                def _():
                    if dist > 1:
                        passing(i, upward, dist - 1, parts[i], owner).wait_recv()
                        passing(i, upward, dist, wholes[i].at[owner], owner).start()
                    else:
                        passing(i, upward, dist, parts[i], owner).start()

        if dist == 1:
            for copy in kept:
                copy.start()

    def end():
        for i in range(len(parts)):
            for upward, last in ((1, size - 1), (0, 0)):
                @pl.when(me == (last if upward else 0))
                def _():
                    for dist in range(1, size):
                        passing(i, upward, dist, parts[i], me).wait_recv()

                for dist in range(1, size):

                    @pl.when(sends(upward, dist))
                    def _():
                        passing(i, upward, dist, parts[i], me).wait_send()

        for copy in kept:
            copy.wait()

    return [lambda dist=dist: step(dist) for dist in range(1, size)], end


def line_spread_steps(size, source, part, whole, place, sems, kept_sem, pieces=4):
    ctx, me = place[0], place[1]
    send_sems, recv_sems = sems
    rows = whole.shape[0] // pieces

    def passing(piece, upward, origin):
        span = pl.ds(piece * rows, rows)
        return pltpu.make_async_remote_copy(
            src_ref=origin.at[span],
            dst_ref=whole.at[span],
            send_sem=send_sems.at[upward, piece],
            recv_sem=recv_sems.at[upward, piece],
            device_id=(ctx, me + (1 if upward else -1)),
            device_id_type=pl.DeviceIdType.MESH,
        )

    kept = pltpu.make_async_copy(part, whole, kept_sem)

    def sends(upward):
        return ((me >= source) & (me < size - 1)) if upward else ((me <= source) & (me > 0))

    def begin():
        for upward in (1, 0):

            @pl.when((me == source) & sends(upward))
            def _():
                for piece in range(pieces):
                    passing(piece, upward, part).start()

        @pl.when(me == source)
        def _():
            kept.start()

    def onward(hops):
        for upward in (1, 0):

            @pl.when((me == source + hops) if upward else (me == source - hops))
            def _():
                for piece in range(pieces):
                    passing(piece, upward, whole).wait_recv()

                    @pl.when(sends(upward))
                    def _():
                        passing(piece, upward, whole).start()

    def end():
        for upward in (1, 0):

            @pl.when(sends(upward))
            def _():
                for piece in range(pieces):
                    passing(piece, upward, whole).wait_send()

        @pl.when(me == source)
        def _():
            kept.wait()

    return [begin] + [lambda hops=hops: onward(hops) for hops in range(1, size)], end


def line_scatter_steps(size, arrays, outs, arrived, running, place, sems):
    ctx, me = place[0], place[1]
    send_sems, recv_sems = sems
    count, rows = len(arrays), outs[0].shape[0]

    def part(i, owner):
        return arrays[i].at[pl.ds(owner * rows, rows)]

    def passing(i, owner, upward, source):
        return pltpu.make_async_remote_copy(
            src_ref=source,
            dst_ref=arrived[i].at[upward, owner],
            send_sem=send_sems.at[i, upward, owner],
            recv_sem=recv_sems.at[i, upward, owner],
            device_id=(ctx, me + (1 if upward else -1)),
            device_id_type=pl.DeviceIdType.MESH,
        )

    def way(step, upward):
        owner = size - 1 - step if upward else step
        return owner, (me < owner) if upward else (me > owner), 0 if upward else size - 1

    def forward(i, step, upward, slot):
        owner, passes, first = way(step, upward)
        passes = passes & ((me if upward else size - 1 - me) == slot - 1 - step)

        @pl.when(passes & (me == first))
        def _():
            passing(i, owner, upward, part(i, owner)).start()

        @pl.when(passes & (me != first))
        def _():
            passing(i, owner, upward, part(i, owner)).wait_recv()
            add_rows(running[i].at[owner], part(i, owner), arrived[i].at[upward, owner], jnp.bfloat16)
            passing(i, owner, upward, running[i].at[owner]).start()

    def turn(slot):
        for i in range(count):
            for upward in (1, 0):
                for step in range(slot):
                    forward(i, step, upward, slot)

    def end():
        for i in range(count):
            for owner in range(size):
                ways = [upward for upward in (1, 0) if owner != (0 if upward else size - 1)]
                for upward in ways:
                    source = part(i, owner) if upward == ways[0] else outs[i]

                    @pl.when(me == owner)
                    def _():
                        passing(i, owner, upward, part(i, owner)).wait_recv()
                        add_rows(outs[i], source, arrived[i].at[upward, owner], jnp.float32)

        for i in range(count):
            for step in range(size - 1):
                for upward in (1, 0):
                    owner, passes, _ = way(step, upward)

                    @pl.when(passes)
                    def _():
                        passing(i, owner, upward, part(i, owner)).wait_send()

    return [lambda slot=slot: turn(slot) for slot in range(size)], end


def greet_line(place, size, peers):
    ctx, me = place[0], place[1]
    barrier = pltpu.get_barrier_semaphore()
    for way, edge in ((-1, 0), (1, size - 1)):

        @pl.when(me != edge)
        def _():
            pl.semaphore_signal(
                barrier, inc=1, device_id=(ctx, me + way), device_id_type=pl.DeviceIdType.MESH
            )

    for peer in peers:
        pl.semaphore_signal(barrier, inc=1, device_id=peer, device_id_type=pl.DeviceIdType.MESH)
    pl.semaphore_wait(barrier, len(peers) + jnp.where((me == 0) | (me == size - 1), 1, 2))


def run_steps(plans):
    longest = max(len(steps) for steps, end in plans)
    for k in range(longest):
        for steps, end in plans:
            if k < len(steps):
                steps[k]()
    for steps, end in plans:
        end()


def dma(*shape):
    return pltpu.SemaphoreType.DMA(shape)


def on_grid():
    return lax.axis_size("ctx") == 8 and lax.axis_size("fsdp") == 4


def plane_gather(parts, ident):
    if lax.axis_size("ctx") != 8:
        return [lax.all_gather(part, "ctx", axis=0, tiled=True) for part in parts]
    count = len(parts)

    def kernel(*refs):
        ins, outs = refs[:count], refs[count : 2 * count]
        place = plane_peers()
        greet(place[2:])
        run_steps([plane_gather_steps(ins, outs, place, refs[2 * count : 2 * count + 2], refs[2 * count + 2])])

    wholes = pl.pallas_call(
        kernel,
        out_shape=[jax.ShapeDtypeStruct((8,) + part.shape, part.dtype) for part in parts],
        in_specs=[pl.BlockSpec(memory_space=pltpu.VMEM)] * count,
        out_specs=[pl.BlockSpec(memory_space=pl.ANY)] * count,
        scratch_shapes=[dma(count * GATHER_COPIES), dma(count * GATHER_COPIES), dma(count)],
        compiler_params=pltpu.CompilerParams(collective_id=ident, has_side_effects=True),
        name="plane_gather",
    )(*parts)
    return [whole.reshape((-1,) + whole.shape[2:]) for whole in wholes]


def first_gather(parts, lined, out_part, ident):
    size = lax.axis_size("fsdp")
    if not on_grid():
        wholes = [lax.all_gather(part, "ctx", axis=0, tiled=True) for part in parts]
        return wholes + [lax.all_gather(part, "fsdp", axis=0) for part in lined] + [None]
    count, extra = len(parts), len(lined)
    total = count + extra + 1

    def kernel(*refs):
        ins, outs = refs[:total], refs[total : 2 * total]
        plane_send, plane_recv, line_send, line_recv, spread_send, spread_recv, kept = refs[2 * total :]
        place = plane_peers()
        source = place[0] * size // 8
        line = (place[0], place[1])
        greet_line(line, size, place[2:])
        run_steps(
            [
                line_gather_steps(
                    size,
                    ins[count : total - 1],
                    outs[count : total - 1],
                    line,
                    (line_send, line_recv),
                    kept.at[pl.ds(count, extra)],
                ),
                line_spread_steps(
                    size, source, ins[-1], outs[-1], line, (spread_send, spread_recv), kept.at[total - 1]
                ),
                plane_gather_steps(ins[:count], outs[:count], place, (plane_send, plane_recv), kept),
            ]
        )

    shapes = [(8,) + part.shape for part in parts] + [(size,) + part.shape for part in lined] + [out_part.shape]
    results = pl.pallas_call(
        kernel,
        out_shape=[jax.ShapeDtypeStruct(shape, jnp.bfloat16) for shape in shapes],
        in_specs=[pl.BlockSpec(memory_space=pltpu.VMEM)] * total,
        out_specs=[pl.BlockSpec(memory_space=pl.ANY)] * total,
        scratch_shapes=[
            dma(count * GATHER_COPIES),
            dma(count * GATHER_COPIES),
            dma(extra, 2, size),
            dma(extra, 2, size),
            dma(2, 4),
            dma(2, 4),
            dma(total),
        ],
        compiler_params=pltpu.CompilerParams(collective_id=ident, has_side_effects=True),
        name="first_gather",
    )(*parts, *lined, out_part)
    wholes = [whole.reshape((-1,) + whole.shape[2:]) for whole in results[:count]]
    return wholes + list(results[count:])


def swap(weights, totals, ident):
    size = lax.axis_size("fsdp")
    if not on_grid():
        return [rows_gathered(weight) for weight in weights], [offloaded_scatter(total) for total in totals]
    given, count = len(weights), len(totals)
    shards = [(total.shape[0] // size, total.shape[1]) for total in totals]

    def kernel(*refs):
        parts, arrays = refs[:given], refs[given : given + count]
        wholes, outs = refs[given + count : 2 * given + count], refs[2 * given + count : 2 * (given + count)]
        arrived, running = (refs[2 * given + k * count : 2 * given + (k + 1) * count] for k in (2, 3))
        gather_send, gather_recv, kept, send_sems, recv_sems = refs[2 * given + 4 * count :]
        place = (lax.axis_index("ctx"), lax.axis_index("fsdp"))
        greet_line(place, size, ())
        run_steps(
            [
                line_gather_steps(size, parts, wholes, place, (gather_send, gather_recv), kept),
                line_scatter_steps(size, arrays, outs, arrived, running, place, (send_sems, recv_sems)),
            ]
        )

    results = pl.pallas_call(
        kernel,
        out_shape=[jax.ShapeDtypeStruct((size,) + weight.shape, weight.dtype) for weight in weights]
        + [jax.ShapeDtypeStruct(shard, jnp.float32) for shard in shards],
        in_specs=[pl.BlockSpec(memory_space=pltpu.VMEM)] * (given + count),
        out_specs=[pl.BlockSpec(memory_space=pl.ANY)] * given + [pl.BlockSpec(memory_space=pltpu.VMEM)] * count,
        scratch_shapes=[pltpu.VMEM((2, size) + shard, jnp.bfloat16) for shard in shards]
        + [pltpu.VMEM((size,) + shard, jnp.bfloat16) for shard in shards]
        + [dma(given, 2, size), dma(given, 2, size), dma(given), dma(count, 2, size), dma(count, 2, size)],
        compiler_params=pltpu.CompilerParams(collective_id=ident, has_side_effects=True),
        name="swap",
    )(*weights, *totals)
    return [whole.reshape(-1, whole.shape[2]) for whole in results[:given]], list(results[given:])


def add_rows(target, left, right, kind, step=32):
    def one(turn, carried):
        rows = pl.ds(pl.multiple_of(turn * step, step), step)
        target[rows] = (left[rows].astype(jnp.float32) + right[rows].astype(jnp.float32)).astype(kind)
        return carried

    lax.fori_loop(0, target.shape[0] // step, one, 0)


def scatter_kernel(total, out, near, sums, far, send_sems, recv_sems):
    sems = (send_sems, recv_sems)
    me, _, core, x, y = plane_peers()
    greet((core, x, y))
    rows = out.shape[0]
    half = rows // 2
    first, last = pl.ds(0, half), pl.ds(half, half)
    flips = (6, 2, 4, 0)
    inward = [send(total.at[me ^ 1 ^ flip], near.at[i], sems, i, core) for i, flip in enumerate(flips)]
    for copy in inward:
        copy.start()
    diagonal_x = send(sums.at[0, first], far.at[0, first], sems, 4, x)
    diagonal_y = send(sums.at[0, last], far.at[0, last], sems, 5, y)
    x_first = send(sums.at[1, first], far.at[1, first], sems, 6, x)
    x_last = send(sums.at[1, last], far.at[1, last], sems, 7, x)
    y_first = send(sums.at[2, first], far.at[2, first], sems, 8, y)
    y_last = send(sums.at[2, last], far.at[2, last], sems, 9, y)
    inward[0].wait_recv()
    add_rows(sums.at[0], total.at[me ^ 6], near.at[0], jnp.bfloat16)
    diagonal_x.start()
    diagonal_y.start()
    inward[1].wait_recv()
    add_rows(sums.at[1], total.at[me ^ 2], near.at[1], jnp.bfloat16)
    x_first.start()
    inward[2].wait_recv()
    add_rows(sums.at[2], total.at[me ^ 4], near.at[2], jnp.bfloat16)
    y_last.start()
    diagonal_x.wait_recv()
    add_rows(sums.at[2, first], sums.at[2, first], far.at[0, first], jnp.bfloat16)
    y_first.start()
    diagonal_y.wait_recv()
    add_rows(sums.at[1, last], sums.at[1, last], far.at[0, last], jnp.bfloat16)
    x_last.start()
    inward[3].wait_recv()
    add_rows(out, total.at[me], near.at[3], jnp.float32)
    x_first.wait_recv()
    add_rows(out.at[first], out.at[first], far.at[1, first], jnp.float32)
    y_last.wait_recv()
    add_rows(out.at[last], out.at[last], far.at[2, last], jnp.float32)
    y_first.wait_recv()
    add_rows(out.at[first], out.at[first], far.at[2, first], jnp.float32)
    x_last.wait_recv()
    add_rows(out.at[last], out.at[last], far.at[1, last], jnp.float32)
    for copy in inward + [diagonal_x, diagonal_y, x_first, x_last, y_first, y_last]:
        copy.wait_send()


def plane_scatter(total, ident):
    total = total.astype(jnp.bfloat16)
    if lax.axis_size("ctx") != 8:
        return lax.psum_scatter(total, "ctx", scatter_dimension=0, tiled=True).astype(jnp.float32)
    rows, width = total.shape[0] // 8, total.shape[1]
    return pl.pallas_call(
        scatter_kernel,
        out_shape=jax.ShapeDtypeStruct((rows, width), jnp.float32),
        in_specs=[pl.BlockSpec(memory_space=pltpu.VMEM)],
        out_specs=pl.BlockSpec(memory_space=pltpu.VMEM),
        scratch_shapes=[
            pltpu.VMEM((4, rows, width), jnp.bfloat16),
            pltpu.VMEM((3, rows, width), jnp.bfloat16),
            pltpu.VMEM((3, rows, width), jnp.bfloat16),
            pltpu.SemaphoreType.DMA((10,)),
            pltpu.SemaphoreType.DMA((10,)),
        ],
        compiler_params=pltpu.CompilerParams(collective_id=ident, has_side_effects=True),
        name="plane_scatter",
    )(total.reshape(8, rows, width))


def offloaded_scatter(total):
    return lax.psum_scatter(
        total.astype(jnp.bfloat16), "fsdp", scatter_dimension=0, tiled=True
    ).astype(jnp.float32)


def gains_kernel(size, parts, out, lined, planed, kept, line_send, line_recv, plane_send, plane_recv):
    me, z = lax.axis_index("ctx"), lax.axis_index("fsdp")
    line = [(me, lax.rem(z + i, size)) for i in range(1, size)]
    plane = [(lax.rem(me + i, 8), z) for i in range(1, 8)]
    greet(line + plane)
    first = [
        send(parts.at[peer[1]], lined.at[i], (line_send, line_recv), i, peer) for i, peer in enumerate(line)
    ]
    for copy in first:
        copy.start()
    for copy in first:
        copy.wait_recv()
    kept[...] = parts[z] + sum(lined[i] for i in range(size - 1))
    second = [send(kept, planed.at[i], (plane_send, plane_recv), i, peer) for i, peer in enumerate(plane)]
    for copy in second:
        copy.start()
    for copy in second:
        copy.wait_recv()
    out[...] = kept[...] + sum(planed[i] for i in range(7))
    for copy in first + second:
        copy.wait_send()


def gains_summed(gains, ident):
    size, place = lax.axis_size("fsdp"), lax.axis_index("fsdp")
    share = gains.shape[1] // size
    if lax.axis_size("ctx") != 8:
        whole = lax.psum(gains, ("ctx", "fsdp"))
        return lax.dynamic_slice_in_dim(whole, place * share, share, 1)
    return pl.pallas_call(
        lambda *refs: gains_kernel(size, *refs),
        out_shape=jax.ShapeDtypeStruct((2, share), jnp.float32),
        in_specs=[pl.BlockSpec(memory_space=pltpu.VMEM)],
        out_specs=pl.BlockSpec(memory_space=pltpu.VMEM),
        scratch_shapes=[
            pltpu.VMEM((size - 1, 2, share), jnp.float32),
            pltpu.VMEM((7, 2, share), jnp.float32),
            pltpu.VMEM((2, share), jnp.float32),
            pltpu.SemaphoreType.DMA((size - 1,)),
            pltpu.SemaphoreType.DMA((size - 1,)),
            pltpu.SemaphoreType.DMA((7,)),
            pltpu.SemaphoreType.DMA((7,)),
        ],
        compiler_params=pltpu.CompilerParams(collective_id=ident, has_side_effects=True),
        name="gains_summed",
    )(gains.reshape(2, size, share).transpose(1, 0, 2))


def together(*values):
    return lax.optimization_barrier(values)


def whole_layer(
    tokens,
    block_order,
    w_query,
    w_key,
    w_value,
    w_out,
    w_gate,
    w_up,
    w_down,
    norm_attn,
    norm_mlp,
    cotangent,
):
    inputs = tokens[0].astype(jnp.float32)
    tok_rows, model_width = inputs.shape
    head_size = HD
    scaling = head_size ** (-0.5)
    layout = block_order[0]
    ctx_size = lax.axis_size("ctx")
    ctx_place = lax.axis_index("ctx")
    seq_rows = tok_rows * ctx_size
    block_rows = seq_rows // layout.shape[0]
    own_heads = HEADS // ctx_size
    share = model_width // ctx_size
    positions = slot_positions(layout, jnp.arange(seq_rows, dtype=jnp.int32), block_rows)
    cosine, sine = rotation_tables(positions, head_size)

    out_part = lax.dynamic_slice_in_dim(w_out, (ctx_place * share) % w_out.shape[0], share, 0)
    seq_tokens, grad_b, w_query, w_key, w_value, gains, out_rows = first_gather(
        [tokens[0], cotangent[0]],
        [own_columns(w, ctx_place, ctx_size) for w in (w_query, w_key, w_value)] + [jnp.stack([norm_attn, norm_mlp])],
        out_part,
        0,
    )
    w_query, w_key, w_value = (w.reshape(model_width, share) for w in (w_query, w_key, w_value))
    if out_rows is None:
        out_cols = rows_gathered(own_columns(w_out, ctx_place, ctx_size))
        out_rows = lax.all_to_all(out_cols, "ctx", split_axis=0, concat_axis=1, tiled=True)
    gains = gains.transpose(1, 0, 2).reshape(2, model_width).astype(jnp.float32)
    gain_attn, gain_mlp = gains[0], gains[1]
    ff_share = w_gate.shape[1] // ctx_size
    ff_half = ff_share // 2
    ff_parts = [
        [
            lax.dynamic_slice_in_dim(w, ctx_place * ff_share + half * ff_half, ff_half, 1)
            for w in (w_gate, w_up, w_down)
        ]
        for half in range(2)
    ]
    ff_first, seq_tokens = together(jnp.concatenate(ff_parts[0], axis=1), seq_tokens)
    ff_first = rows_gathered(ff_first)

    scale_attn = rms_scale(inputs)
    normed_attn = inputs * scale_attn
    seq_inputs = seq_tokens.astype(jnp.float32)
    hidden_attn = (seq_inputs * rms_scale(seq_inputs) * gain_attn[None, :]).astype(jnp.bfloat16)
    query, keyed, valued = (
        jnp.dot(hidden_attn, w, preferred_element_type=jnp.float32).reshape(seq_rows, own_heads, head_size)
        for w in (w_query, w_key, w_value)
    )
    query_rot = rotate(query, cosine, sine).astype(jnp.bfloat16)
    key_rot = rotate(keyed, cosine, sine).astype(jnp.bfloat16)
    value_b = valued.astype(jnp.bfloat16)
    allowed = (positions[None, :] <= positions[:, None])[None]
    scores = jnp.einsum("qhd,khd->hqk", query_rot, key_rot, preferred_element_type=jnp.float32) * scaling
    maxima = jnp.max(jnp.where(allowed, scores, neg_large), axis=-1)
    probs = jnp.where(allowed, jnp.exp(scores - maxima[..., None]), 0.0)
    totals = jnp.sum(probs, axis=-1)
    mixed = jnp.einsum("hqk,khd->qhd", probs.astype(jnp.bfloat16), value_b, preferred_element_type=jnp.float32)
    attn_rows = (mixed / totals.T[:, :, None]).astype(jnp.bfloat16).reshape(seq_rows, share)
    log_totals = maxima + jnp.log(totals)

    mid_stream = inputs + plane_scatter(jnp.dot(attn_rows, out_rows, preferred_element_type=jnp.float32), 1)
    scale_mlp = rms_scale(mid_stream)
    normed_mlp = mid_stream * scale_mlp
    (hidden_mlp,) = plane_gather([(normed_mlp * gain_mlp[None, :]).astype(jnp.bfloat16)], 2)
    acted, grad_gate_pre, grad_up_pre = [], [], []
    ff_whole = [jnp.split(ff_first, 3, axis=1)]
    for half in range(2):
        gate_cols, up_cols, down_cols = ff_whole[half]
        gate_pre = jnp.dot(hidden_mlp, gate_cols, preferred_element_type=jnp.float32)
        up_pre = jnp.dot(hidden_mlp, up_cols, preferred_element_type=jnp.float32)
        grad_act = jnp.dot(grad_b, down_cols, preferred_element_type=jnp.float32)
        sigmoid_gate = jax.nn.sigmoid(gate_pre)
        silu_gate = gate_pre * sigmoid_gate
        acted.append((silu_gate * up_pre).astype(jnp.bfloat16))
        grad_gate_pre.append(
            (grad_act * up_pre * sigmoid_gate * (1.0 + gate_pre * (1.0 - sigmoid_gate))).astype(jnp.bfloat16)
        )
        grad_up_pre.append((grad_act * silu_gate).astype(jnp.bfloat16))
        if half == 0:
            parts = [
                contract_rows(grad_b, acted[0]).astype(jnp.bfloat16),
                contract_rows(hidden_mlp, grad_gate_pre[0]).astype(jnp.bfloat16),
                contract_rows(hidden_mlp, grad_up_pre[0]).astype(jnp.bfloat16),
            ]
            second, first_grads = swap(ff_parts[1], parts, 7)
            ff_whole.append(second)
        else:
            parts = [
                contract_rows(grad_b, acted[1]).astype(jnp.bfloat16),
                contract_rows(
                    hidden_mlp, jnp.concatenate([grad_gate_pre[1], grad_up_pre[1]], axis=1)
                ).astype(jnp.bfloat16),
            ]
    parts[0], parts[1], grad_gate_pre[1], grad_up_pre[1], acted[1] = together(
        parts[0], parts[1], grad_gate_pre[1], grad_up_pre[1], acted[1]
    )
    second_grads = [offloaded_scatter(parts[0]), offloaded_scatter(parts[1])]
    grad_down = jnp.concatenate([first_grads[0], second_grads[0]], axis=1)
    grad_gate = jnp.concatenate([first_grads[1], second_grads[1][:, :ff_half]], axis=1)
    grad_up = jnp.concatenate([first_grads[2], second_grads[1][:, ff_half:]], axis=1)
    columns = plane_scatter(
        sum(
            contract_last(grad_gate_pre[half], ff_whole[half][0]) + contract_last(grad_up_pre[half], ff_whole[half][1])
            for half in range(2)
        ),
        4,
    )
    gain_grad_mlp = jnp.sum(columns * normed_mlp, axis=0)
    grad_mid = cotangent[0].astype(jnp.float32) + norm_back(
        columns * gain_mlp[None, :], normed_mlp, scale_mlp
    )
    (grad_mid_b,) = plane_gather([grad_mid.astype(jnp.bfloat16)], 5)
    attn_all = lax.all_gather(attn_rows, "ctx", axis=1, tiled=True)
    part_out = contract_rows(attn_all, own_columns(grad_mid_b, ctx_place, ctx_size)).astype(jnp.bfloat16)
    part_out, grad_mid_b = together(part_out, grad_mid_b)
    grad_out = offloaded_scatter(part_out)
    grad_attn = contract_last(grad_mid_b, out_rows).astype(jnp.bfloat16)
    delta = jnp.sum(
        (grad_attn.astype(jnp.float32) * attn_rows.astype(jnp.float32)).reshape(
            seq_rows, own_heads, head_size
        ),
        axis=-1,
    ).T
    grad_heads = grad_attn.reshape(seq_rows, own_heads, head_size)
    probs = jnp.where(allowed, jnp.exp(scores - log_totals[..., None]), 0.0)
    grad_v = jnp.einsum("hqk,qhd->khd", probs.astype(jnp.bfloat16), grad_heads, preferred_element_type=jnp.float32)
    grad_probs = jnp.einsum("qhd,khd->hqk", grad_heads, value_b, preferred_element_type=jnp.float32)
    grad_scores = (probs * (grad_probs - delta[..., None]) * scaling).astype(jnp.bfloat16)
    grad_q = jnp.einsum("hqk,khd->qhd", grad_scores, key_rot, preferred_element_type=jnp.float32)
    grad_k = jnp.einsum("hqk,qhd->khd", grad_scores, query_rot, preferred_element_type=jnp.float32)
    grad_q, grad_k, grad_v = (
        grad.astype(jnp.bfloat16).reshape(seq_rows, share)
        for grad in (rotate_back(grad_q, cosine, sine), rotate_back(grad_k, cosine, sine), grad_v)
    )
    part_qkv = contract_rows(hidden_attn, jnp.concatenate([grad_q, grad_k, grad_v], axis=1)).astype(jnp.bfloat16)
    part_qkv, grad_q, grad_k, grad_v = together(part_qkv, grad_q, grad_k, grad_v)
    grads_qkv = offloaded_scatter(part_qkv)
    columns = plane_scatter(
        contract_last(grad_q, w_query) + contract_last(grad_k, w_key) + contract_last(grad_v, w_value), 6
    )
    summed = sum(contract_last(acted[half], ff_whole[half][2]) for half in range(2)).astype(jnp.bfloat16)
    summed, columns = together(summed, columns)
    result = mid_stream + plane_scatter(summed, 3)
    gain_grad_attn = jnp.sum(columns * normed_attn, axis=0)
    grad_input = grad_mid + norm_back(columns * gain_attn[None, :], normed_attn, scale_attn)
    gain_own = gains_summed(jnp.stack([gain_grad_attn, gain_grad_mlp]), 8)
    return (
        result[None],
        grad_input[None],
        grads_qkv[:, :share],
        grads_qkv[:, share : 2 * share],
        grads_qkv[:, 2 * share :],
        grad_out,
        grad_gate,
        grad_up,
        grad_down,
        gain_own[0],
        gain_own[1],
    )


def solution(mesh):
    in_specs = (
        P("fsdp", "ctx", None),
        P("fsdp", None),
        P("fsdp", None),
        P("fsdp", None),
        P("fsdp", None),
        P("fsdp", None),
        P("fsdp", None),
        P("fsdp", None),
        P("fsdp", None),
        P("fsdp"),
        P("fsdp"),
        P("fsdp", "ctx", None),
    )
    out_specs = (
        P("fsdp", "ctx", None),
        P("fsdp", "ctx", None),
        P("fsdp", "ctx"),
        P("fsdp", "ctx"),
        P("fsdp", "ctx"),
        P("fsdp", "ctx"),
        P("fsdp", "ctx"),
        P("fsdp", "ctx"),
        P("fsdp", "ctx"),
        P("fsdp"),
        P("fsdp"),
    )
    return jax.shard_map(whole_layer, mesh=mesh, in_specs=in_specs, out_specs=out_specs, check_vma=False)
```
